32 devices in a mesh: dp: 4 (over x, core), param: 8 (over z, y).
Axes of the slice: x: 2, y: 2, z: 4, core: 2. Of those that a mesh axis runs over, the one named last changes fastest.
Arguments:
- train_grads: bfloat16 [3584, 212992], P('dp', 'param'), as said below
- query_grads: bfloat16 [128, 212992], P('dp', 'param'), as said below
Outputs:
- scores: float32 [128, 3584], P('param', 'dp')
Inputs may be any that keep to these rules, and one draw needn't show every extreme that they name: `train_grads`: finite real values. `query_grads`: finite real values.
All inputs are finite; a program needn't handle non-finite values.
Results may differ from the reference program's by a relative error of at most 0.0003.
Values may be sent and summed in bfloat16 or wider, within the bound.
A program may use at most 128 MiB of HBM per device.

```python
import math
import jax
import jax.numpy as jnp
from jax import lax

TR_DEV = 896
GRAD = 212992
NTR = 3584
NQ = 128
N_DP = 4


latent_count = 256


decay_power = 0.35


def shared_basis(key):
    base = jax.random.fold_in(key, 7)
    spread = jax.random.uniform(jax.random.fold_in(base, 1), (GRAD,), jnp.float32)
    column_scale = jnp.exp(math.log(10.0) * spread) * (1.0 + 2.0 * jnp.arange(GRAD, dtype=jnp.float32) / GRAD)
    basis = jax.random.normal(jax.random.fold_in(base, 2), (latent_count, GRAD), jnp.float32)
    return (column_scale, basis)


def make_grads(key, salt, row_count):
    column_scale, basis = shared_basis(key)
    inner = jax.random.fold_in(key, salt)
    decay = jnp.power(jnp.arange(latent_count, dtype=jnp.float32) + 1.0, -decay_power)
    decay = decay / jnp.sqrt(jnp.sum(decay * decay))
    weights = jax.random.normal(jax.random.fold_in(inner, 1), (row_count, latent_count), jnp.float32) * decay[None, :]
    noise = jax.random.normal(jax.random.fold_in(inner, 2), (row_count, GRAD), jnp.float32)
    spread = jax.random.uniform(jax.random.fold_in(inner, 3), (row_count,), jnp.float32)
    mixed = jnp.dot(weights, basis) + 0.5 * noise
    row_scale = jnp.exp(math.log(10.0) * spread)
    return (row_scale[:, None] * column_scale[None, :] * mixed).astype(jnp.bfloat16)


def draw_train_grads(key, part):
    return make_grads(key, 11, NTR)


def draw_query_grads(key, part):
    return make_grads(key, 13, NQ)


def setup_inputs(seed: int = 0) -> dict:
    splits = jax.random.split(jax.random.key(seed), 3)
    return {
        "train_grads": draw_train_grads(jax.random.fold_in(splits[2], 71), 0),
        "query_grads": draw_query_grads(jax.random.fold_in(splits[2], 71), 0),
    }


epsilon = 1e-06

def reference(train_grads, query_grads):
    query_norm = lax.optimization_barrier(jnp.sum(jnp.square(query_grads.astype(jnp.float32)), axis=1))
    blocks = train_grads.reshape(N_DP, TR_DEV, GRAD)

    def one_block(block):
        products = lax.dot_general(query_grads, block, (((1,), (1,)), ((), ())), preferred_element_type=jnp.float32)
        block_norm = lax.optimization_barrier(jnp.sum(jnp.square(block.astype(jnp.float32)), axis=1))
        return (products, block_norm)
    products, train_norm = lax.map(one_block, blocks)
    products = jnp.transpose(products, (1, 0, 2)).reshape(NQ, NTR)
    train_norm = train_norm.reshape(NTR)
    return products * lax.rsqrt(query_norm + epsilon)[:, None] * lax.rsqrt(train_norm + epsilon)[None, :]
```

```python
import functools

import jax
import jax.numpy as jnp
from jax import lax
from jax.experimental import pallas as pl
from jax.experimental.pallas import tpu as pltpu
from jax.sharding import PartitionSpec as P

epsilon = 1e-06
lanes = 128
max_chunk = 2048
ahead = 2
block_rows = 256


def chunk_width(width):
    best = lanes
    for tiles in range(1, max_chunk // lanes + 1):
        if width % (tiles * lanes) == 0:
            best = tiles * lanes
    return best


def nt_dot(a, b):
    return lax.dot_general(a, b, (((1,), (1,)), ((), ())), preferred_element_type=jnp.float32)


def kernel(
    cfg, train_hbm, query_hbm, out_ref,
    train, first_q, second_q, first_sum, second_sum, norm_sum, parts, norm_parts,
    train_sem, self_sem, x_send, x_recv, mate_send, mate_recv, fwd_send, fwd_recv,
    part_send, part_recv, norm_send, norm_recv,
):
    chips, params, chunks, width, rows, unit, count, owned, piece = cfg
    dp = lax.axis_index("dp")
    me = lax.axis_index("param")
    chip, core = dp // 2, lax.rem(dp, 2)
    mate = chip * 2 + (1 - core)
    base = 2 * rows
    steps = 2 * chunks

    def columns(c):
        return pl.ds(pl.multiple_of(c * width, width), width)

    def train_copy(c):
        return pltpu.make_async_copy(train_hbm.at[:, columns(c)], train.at[c], train_sem.at[c])

    def self_copy(c):
        return pltpu.make_async_copy(
            query_hbm.at[:, columns(c)], first_q.at[c, pl.ds(0, rows), :], self_sem.at[c]
        )

    def mate_copy(c):
        return pltpu.make_async_remote_copy(
            src_ref=query_hbm.at[:, columns(c)],
            dst_ref=first_q.at[c, pl.ds(rows, rows), :],
            send_sem=mate_send.at[c],
            recv_sem=mate_recv.at[c],
            device_id={"dp": mate},
        )

    def slot(group, c, place):
        if group == 0:
            return first_q.at[c, pl.ds(base + unit * place, unit), :]
        return second_q.at[c, pl.ds(unit * place, unit), :]

    def x_copy(group, c, d):
        start = pl.multiple_of(lax.rem(group + core, 2) * unit, unit)
        return pltpu.make_async_remote_copy(
            src_ref=query_hbm.at[pl.ds(start, unit), columns(c)],
            dst_ref=slot(group, c, 2 * (d - 1)),
            send_sem=x_send.at[d - 1, group * chunks + c],
            recv_sem=x_recv.at[d - 1, group * chunks + c],
            device_id={"dp": lax.rem(chip + d, chips) * 2 + core},
        )

    def fwd_copy(group, c, d):
        return pltpu.make_async_remote_copy(
            src_ref=slot(group, c, 2 * (d - 1)),
            dst_ref=slot(group, c, 2 * (d - 1) + 1),
            send_sem=fwd_send.at[d - 1, group * chunks + c],
            recv_sem=fwd_recv.at[d - 1, group * chunks + c],
            device_id={"dp": mate},
        )

    def pump(group, c):
        for d in range(1, chips):
            x_copy(group, c, d).wait_recv()
            fwd_copy(group, c, d).start()

    def piece_list(group):
        out = []
        if group == 0:
            for source, at in ((dp, 0), (mate, rows)):
                for r in range(0, rows, piece):
                    out.append((first_sum, at + r, source * rows + r))
        for d in range(1, chips):
            other = lax.rem(chip - d + chips, chips)
            for k in range(2):
                from_core = core if k == 0 else 1 - core
                start = lax.rem(group + from_core, 2) * unit
                at = unit * (2 * (d - 1) + k)
                for r in range(0, unit, piece):
                    row = (other * 2 + from_core) * rows + start + r
                    if group == 0:
                        out.append((first_sum, base + at + r, row))
                    else:
                        out.append((second_sum, at + r, row))
        return out

    first_pieces, second_pieces = piece_list(0), piece_list(1)

    def part_copy(index, item):
        buffer, at, row = item
        owner, offset = row // owned, lax.rem(row, owned)
        return owner, offset, pltpu.make_async_remote_copy(
            src_ref=buffer.at[pl.ds(at, piece), :],
            dst_ref=parts.at[me, pl.ds(pl.multiple_of(offset, piece), piece), :],
            send_sem=part_send.at[index],
            recv_sem=part_recv.at[me, offset // piece],
            device_id={"param": owner},
        )

    def send_parts(first_index, items):
        for i, item in enumerate(items):
            owner, offset, copy = part_copy(first_index + i, item)

            @pl.when(owner != me)
            def _():
                copy.start()

            @pl.when(owner == me)
            def _():
                buffer, at, _row = item
                parts[me, pl.ds(pl.multiple_of(offset, piece), piece), :] = buffer[pl.ds(at, piece), :]

    def wait_parts_sent(first_index, items):
        for i, item in enumerate(items):
            owner, _offset, copy = part_copy(first_index + i, item)

            @pl.when(owner != me)
            def _():
                copy.wait_send()

    def norm_copy(j):
        return pltpu.make_async_remote_copy(
            src_ref=norm_parts.at[me],
            dst_ref=norm_parts.at[me],
            send_sem=norm_send.at[j],
            recv_sem=norm_recv.at[me],
            device_id={"param": lax.rem(me + j, params)},
        )

    @pl.loop(0, chunks)
    def _(c):
        train_copy(c).start()
        self_copy(c).start()

    barrier = pltpu.get_barrier_semaphore()
    pl.semaphore_signal(barrier, inc=1, device_id={"dp": mate})
    for d in range(1, chips):
        pl.semaphore_signal(barrier, inc=1, device_id={"dp": lax.rem(chip + d, chips) * 2 + core})
    for j in range(1, params):
        pl.semaphore_signal(barrier, inc=1, device_id={"param": lax.rem(me + j, params)})
    pl.semaphore_wait(barrier, chips + params - 1)

    @pl.loop(0, chunks)
    def _(c):
        for d in range(1, chips):
            x_copy(0, c, d).start()
        mate_copy(c).start()

    @pl.loop(0, chunks)
    def _(c):
        for d in range(1, chips):
            x_copy(1, c, d).start()

    first_sum[...] = jnp.zeros_like(first_sum)
    second_sum[...] = jnp.zeros_like(second_sum)
    norm_sum[...] = jnp.zeros_like(norm_sum)

    def add_query_norm(total, q):
        acc = total[:, pl.ds(count, lanes)]
        for k in range(0, width, lanes):
            x = q[:, k : k + lanes].astype(jnp.float32)
            acc = acc + x * x
        total[:, pl.ds(count, lanes)] = acc

    for c in range(ahead):
        pump(0, c)

    @pl.loop(0, chunks)
    def _(c):
        @pl.when(c + ahead < chunks)
        def _():
            pump(0, c + ahead)

        @pl.when(c + ahead >= chunks)
        def _():
            pump(1, c + ahead - chunks)

        train_copy(c).wait()
        self_copy(c).wait()
        mate_copy(c).wait_recv()
        for d in range(1, chips):
            fwd_copy(0, c, d).wait_recv()
        q = first_q[c]
        add_query_norm(first_sum, q)
        for r in range(0, count, block_rows):
            size = min(block_rows, count - r)
            t = train[c, pl.ds(r, size), :]
            first_sum[:, pl.ds(r, size)] += nt_dot(q, t)
            for s in range(0, size, lanes):
                acc = norm_sum[pl.ds(r + s, lanes), :]
                for k in range(0, width, lanes):
                    x = t[s : s + lanes, k : k + lanes].astype(jnp.float32)
                    acc = acc + x * x
                norm_sum[pl.ds(r + s, lanes), :] = acc

    totals = [
        jnp.sum(norm_sum[pl.ds(r, lanes), :].T, axis=0, keepdims=True) for r in range(0, count, lanes)
    ]
    spare = norm_parts.shape[1] - len(totals)
    if spare:
        totals.append(jnp.zeros((spare, lanes), jnp.float32))
    norm_parts[me] = jnp.concatenate(totals, axis=0)
    send_parts(0, first_pieces)
    for j in range(1, params):
        norm_copy(j).start()

    @pl.loop(0, chunks)
    def _(c):
        @pl.when(c + ahead < chunks)
        def _():
            pump(1, c + ahead)

        for d in range(1, chips):
            fwd_copy(1, c, d).wait_recv()
        q = second_q[c]
        add_query_norm(second_sum, q)
        for r in range(0, count, block_rows):
            size = min(block_rows, count - r)
            second_sum[:, pl.ds(r, size)] += nt_dot(q, train[c, pl.ds(r, size), :])

    send_parts(len(first_pieces), second_pieces)

    @pl.loop(0, chunks)
    def _(c):
        mate_copy(c).wait_send()
        for d in range(1, chips):
            for group in range(2):
                x_copy(group, c, d).wait_send()
                fwd_copy(group, c, d).wait_send()

    norm = norm_parts[me]
    for j in range(1, params):
        other = lax.rem(me + j, params)
        pltpu.make_async_copy(norm_parts.at[other], norm_parts.at[other], norm_recv.at[other]).wait()
        norm = norm + norm_parts[other]
        norm_copy(j).wait_send()
    train_scale = lax.rsqrt(norm + epsilon)

    total = parts[me]
    for j in range(1, params):
        other = lax.rem(me + j, params)
        for k in range(owned // piece):
            place = parts.at[other, pl.ds(k * piece, piece), :]
            pltpu.make_async_copy(place, place, part_recv.at[other, k]).wait()
        total = total + parts[other]
    query_norm = jnp.sum(total[:, count:], axis=1, keepdims=True)
    query_scale = lax.rsqrt(query_norm + epsilon)
    for k in range(count // lanes):
        at = slice(k * lanes, (k + 1) * lanes)
        out_ref[:, at] = total[:, at] * query_scale * train_scale[k : k + 1, :]

    wait_parts_sent(0, first_pieces)
    wait_parts_sent(len(first_pieces), second_pieces)


def solution(mesh):
    chips, params = mesh.shape["dp"] // 2, mesh.shape["param"]

    def per_device(train_grads, query_grads):
        count, total = train_grads.shape
        rows = query_grads.shape[0]
        width = chunk_width(total)
        chunks = total // width
        unit = rows // 2
        owned = rows * chips * 2 // params
        piece = min(unit, owned)
        far = 2 * (chips - 1) * unit
        pieces = (2 * rows + 2 * far) // piece
        cfg = (chips, params, chunks, width, rows, unit, count, owned, piece)
        dma = pltpu.SemaphoreType.DMA
        return pl.pallas_call(
            functools.partial(kernel, cfg),
            out_shape=jax.ShapeDtypeStruct((owned, count), jnp.float32),
            in_specs=[pl.BlockSpec(memory_space=pl.ANY)] * 2,
            out_specs=pl.BlockSpec(memory_space=pltpu.VMEM),
            scratch_shapes=[
                pltpu.VMEM((chunks, count, width), jnp.bfloat16),
                pltpu.VMEM((chunks, 2 * rows + far, width), jnp.bfloat16),
                pltpu.VMEM((chunks, far, width), jnp.bfloat16),
                pltpu.VMEM((2 * rows + far, count + lanes), jnp.float32),
                pltpu.VMEM((far, count + lanes), jnp.float32),
                pltpu.VMEM((count, lanes), jnp.float32),
                pltpu.VMEM((params, owned, count + lanes), jnp.float32),
                pltpu.VMEM((params, -(-count // lanes // 8) * 8, lanes), jnp.float32),
                dma((chunks,)),
                dma((chunks,)),
                dma((chips - 1, 2 * chunks)),
                dma((chips - 1, 2 * chunks)),
                dma((chunks,)),
                dma((chunks,)),
                dma((chips - 1, 2 * chunks)),
                dma((chips - 1, 2 * chunks)),
                dma((pieces,)),
                dma((params, owned // piece)),
                dma((params,)),
                dma((params,)),
            ],
            compiler_params=pltpu.CompilerParams(
                collective_id=0, has_side_effects=True, vmem_limit_bytes=62 * 1024 * 1024
            ),
        )(train_grads, query_grads)

    return jax.shard_map(
        per_device,
        mesh=mesh,
        in_specs=(P("dp", "param"), P("dp", "param")),
        out_specs=P("param", "dp"),
        check_vma=False,
    )
```
